32 devices in a mesh: parts: 2 (over y), dp: 8 (over z, x), tensor: 2 (over core).
Axes of the slice: x: 2, y: 2, z: 4, core: 2. Of those that a mesh axis runs over, the one named last changes fastest.
Arguments:
- normed: bfloat16 [16, 256, 4096], P(('parts', 'dp')), parts along dimension 0, may hold values from -28 to 28
- q_weight: bfloat16 [4096, 2048], P('dp', 'tensor'), may hold values from -0.09375 to 0.09375
- kv_weight: bfloat16 [4096, 2, 512], P('dp', None, 'tensor'), may hold values from -0.09375 to 0.09375
- o_weight: bfloat16 [2048, 4096], P('tensor', 'dp'), may hold values from -0.5 to 0.5
- lengths: int32 [16], P(('parts', 'dp')), parts along dimension 0, may hold values from 64 to 256
- destinations: int32 [16], P(('parts', 'dp')), parts along dimension 0, may hold values from 0 to 7, each once
Outputs:
- projected: bfloat16 [16, 256, 4096], P(('parts', 'dp'), None, 'tensor'), parts along dimension 0
- kv_cache: bfloat16 [16, 2, 4, 256, 128], P(('parts', 'dp'), None, None, 'tensor'), parts along dimension 0
The draws below stay inside these ranges and needn't reach their ends.
There are 2 independent parts, one for each index of `parts`. The reference program is written for one: setup_inputs(seed, part) draws one part's arguments, and reference() takes and returns one part's arrays. A program takes and returns all parts, laid end to end along the dimension named above; an argument that names none is the same for every part. Nothing has to cross between parts.
All inputs are finite; a program needn't handle non-finite values.
Results may differ from the reference program's by a relative error of at most 0.012.
The reference program's roundings to bfloat16 on the way (of `query`, `keys`, `weights`, `attended` and `cache`) count: a program that leaves them out, or rounds other values in their place, can miss the bound.
Values may be sent and summed in bfloat16 or wider, within the bound.
A program may use at most 128 MiB of HBM per device.

```python
import math
import jax
import jax.numpy as jnp
from jax import lax

D = 4096
HD = 128
HEADS = 16
KV_HEADS = 4
LEN = 256
PROMPTS = 8


def draw_normed(key, part):
    shape = (PROMPTS, LEN, D)
    base_key = jax.random.fold_in(key, 11)
    values = jax.random.truncated_normal(base_key, -6.0, 6.0, shape, jnp.float32)
    return values.astype(jnp.bfloat16)


def touch_ends(drawn, stream_key, low, high):
    dims = drawn.shape
    place = [jax.random.randint(jax.random.fold_in(stream_key, axis), (), 0, dims[axis]) for axis in range(len(dims))]
    drawn = drawn.at[tuple(place)].set(low)
    longest = dims.index(max(dims))
    place[longest] = (place[longest] + 1) % dims[longest]
    return drawn.at[tuple(place)].set(high)


def level_of(key, extent, split, smallest, top_value):
    factor_of = 1.0
    for dim, blocks in split:
        draws = jax.random.uniform(jax.random.fold_in(jax.random.fold_in(key, 6), dim), (blocks,), jnp.float32, smallest / len(split), top_value / len(split))
        factor_of = factor_of * jnp.repeat(jnp.exp(draws), extent[dim] // blocks).reshape((-1,) + (1,) * (len(extent) - 1 - dim))
    return factor_of


def scatter_about(stream_key, shape, deviation, bound, shards=(), kind=jnp.bfloat16):
    loudness = level_of(stream_key, shape, shards, -0.22, 0.18) if shards else 1.0
    result = jax.random.normal(stream_key, shape, jnp.float32) * deviation * loudness
    return jnp.minimum(jnp.maximum(result, -bound), bound).astype(kind)


def setup_inputs(seed: int = 0, part: int = 0) -> dict:
    key_list = jax.random.split(jax.random.key(seed), 7)
    part_splits = jax.random.split(jax.random.fold_in(key_list[6], part), 7)
    normed = draw_normed(jax.random.fold_in(jax.random.fold_in(key_list[6], part), 71), part)
    q_weight = scatter_about(key_list[1], (D, HEADS * HD), D ** -0.5, 0.09375, ((0, 8), (1, 2)))
    kv_weight = scatter_about(key_list[2], (D, 2, KV_HEADS * HD), D ** -0.5, 0.09375, ((0, 8), (2, 2)))
    o_weight = scatter_about(key_list[3], (HEADS * HD, D), HD ** -0.5, 0.5, ((0, 2), (1, 8)))
    lengths = touch_ends(jax.random.randint(part_splits[4], (PROMPTS,), LEN // 4, LEN + 1), jax.random.fold_in(part_splits[4], 1), LEN // 4, LEN).astype(jnp.int32)
    destinations = jax.random.permutation(part_splits[5], PROMPTS).astype(jnp.int32)
    return dict(normed=normed, q_weight=q_weight, kv_weight=kv_weight, o_weight=o_weight, lengths=lengths, destinations=destinations)


ROPE_BASE = 500000.0

def rotate(values, positions):
    half = values.shape[-1] // 2
    steps = jnp.arange(half, dtype=jnp.float32) * (2.0 / values.shape[-1])
    freq = jnp.power(jnp.float32(ROPE_BASE), -steps)
    angle = positions.astype(jnp.float32)[:, None] * freq[None, :]
    cosine = jnp.cos(angle)[:, None, :]
    sine = jnp.sin(angle)[:, None, :]
    first = values[..., :half]
    second = values[..., half:]
    return jnp.concatenate([first * cosine - second * sine, second * cosine + first * sine], axis=-1)

def reference(normed, q_weight, kv_weight, o_weight, lengths, destinations):

    def one_prompt(item):
        tokens, length = item
        total = tokens.shape[0]
        positions = jnp.arange(total, dtype=jnp.int32)
        query = jnp.dot(tokens, q_weight, preferred_element_type=jnp.float32).reshape(total, HEADS, HD)
        query = rotate(query, positions).astype(jnp.bfloat16)
        pair = jnp.dot(tokens, kv_weight.reshape(D, 2 * KV_HEADS * HD), preferred_element_type=jnp.float32)
        pair = pair.reshape(total, 2, KV_HEADS, HD)
        keys = rotate(pair[:, 0], positions).astype(jnp.bfloat16)
        values = pair[:, 1].astype(jnp.bfloat16)
        group = HEADS // KV_HEADS
        grouped = query.reshape(total, KV_HEADS, group, HD).transpose(1, 2, 0, 3).astype(jnp.float32)
        key_rows = keys.transpose(1, 0, 2).astype(jnp.float32)
        value_rows = values.transpose(1, 0, 2).astype(jnp.float32)
        scores = jnp.einsum('kgqd,ktd->kgqt', grouped, key_rows, precision=lax.Precision.HIGHEST) / math.sqrt(HD)
        allowed = (positions[:, None] >= positions[None, :]) & (positions[None, :] < length)
        scores = jnp.where(allowed, scores, -jnp.inf)
        peak = lax.optimization_barrier(jnp.max(scores, axis=-1, keepdims=True))
        expo = jnp.exp(scores - peak)
        weights = (expo / lax.optimization_barrier(jnp.sum(expo, axis=-1, keepdims=True))).astype(jnp.bfloat16)
        attended = jnp.einsum('kgqt,ktd->kgqd', weights.astype(jnp.float32), value_rows, precision=lax.Precision.HIGHEST)
        attended = attended.astype(jnp.bfloat16).transpose(2, 0, 1, 3).reshape(total, HEADS * HD)
        projected = jnp.dot(attended, o_weight, preferred_element_type=jnp.float32).astype(jnp.bfloat16)
        live = (positions < length)[:, None, None]
        kept_keys = jnp.where(live, keys, jnp.zeros_like(keys))
        kept_values = jnp.where(live, values, jnp.zeros_like(values))
        cache = jnp.stack([kept_keys, kept_values], axis=0).transpose(0, 2, 1, 3)
        return (projected, cache)
    projected, caches = lax.map(one_prompt, (normed, lengths))
    slots = jnp.arange(PROMPTS, dtype=jnp.int32)
    match = destinations[None, :] == slots[:, None]
    source = lax.optimization_barrier(jnp.sum(jnp.where(match, slots[None, :], 0), axis=1)).astype(jnp.int32)
    return (projected, jnp.take(caches, source, axis=0))
```

```python
import functools
import math

import jax
import jax.numpy as jnp
from jax import lax
from jax.experimental import pallas as pl
from jax.experimental.pallas import tpu as pltpu
from jax.sharding import PartitionSpec as P

HD = 128
ROPE_BASE = 500000.0
MESH = pl.DeviceIdType.MESH
F32 = jnp.float32
BF16 = jnp.bfloat16


def tables(total):
    half = HD // 2
    steps = jnp.arange(half, dtype=F32) * (2.0 / HD)
    freq = jnp.power(jnp.float32(ROPE_BASE), -steps)
    angle = jnp.arange(total, dtype=F32)[:, None] * freq[None, :]
    cosine, sine = jnp.cos(angle), jnp.sin(angle)
    return (
        jnp.concatenate([cosine, cosine], axis=1),
        jnp.concatenate([-sine, sine], axis=1),
    )


def rdma(src, dst, send, recv, **device):
    return pltpu.make_async_remote_copy(
        src_ref=src, dst_ref=dst, send_sem=send, recv_sem=recv,
        device_id=device, device_id_type=MESH,
    )


def kernel(n, groups, group, length_ref, dest_ref, tok, w, o, cos_ref, sin_ref,
           out, cache,
           wbuf, obuf, ptok, acc, psend, precv, asend, arecv, dsend, drecv,
           xsend, xrecv, csend, cflat, spread, going, final, dmine, dall, kbuf,
           wz, wr, wl, wy, wys, oz, orr, ol, oy, oys,
           ts, tr, ps, pr, as_, ar, ds, dr, xs, xr, cs, cr,
           des, der, p1s, p1r, p2s, p2r):
    me = lax.axis_index("dp")
    y = lax.axis_index("parts")
    t = lax.axis_index("tensor")
    z = me // 2
    x = me % 2
    links = n // 2
    mate = z * 2 + (1 - x)
    total = tok.shape[1]
    subs, osubs = w.shape[1], o.shape[1]
    width = group * HD
    block = width + 2 * HD
    half = total // 2
    piece = spread.shape[1]
    homes = links // 2

    barrier = pltpu.get_barrier_semaphore()

    def greet(k, c):
        pl.semaphore_signal(
            barrier, inc=1, device_id={"dp": (me + k) % n}, device_id_type=MESH)
        return c

    lax.fori_loop(1, n, greet, 0)
    pl.semaphore_signal(barrier, inc=1, device_id={"tensor": 1 - t}, device_id_type=MESH)
    pl.semaphore_signal(barrier, inc=1, device_id={"parts": 1 - y}, device_id_type=MESH)
    pl.semaphore_wait(barrier, n + 1)

    class Chain:
        def __init__(self, own, buf, zr, sr, sl, yr, ys, count):
            self.own, self.buf, self.count = own, buf, count
            self.zr, self.sr, self.sl, self.yr, self.ys = zr, sr, sl, yr, ys

        def right(self, a, j, src):
            return rdma(src, self.buf.at[a, y, j], self.sr.at[a, j], self.zr.at[a, j], dp=me + 2)

        def left(self, a, j, src):
            return rdma(src, self.buf.at[a, y, j], self.sl.at[a, j], self.zr.at[a, j], dp=me - 2)

        def across(self, a, j, side):
            part = self.buf.at[a, side, j]
            return rdma(part, part, self.ys.at[a, j], self.yr.at[a, j], parts=1 - y)

        def start_right(self):
            for j in range(self.count):
                self.right(z, j, self.own.at[y, j]).start()

        def start_left(self):
            for j in range(self.count):
                self.left(z, j, self.own.at[y, j]).start()

        def forward(self, s):
            a, b = z - s, z + s
            for j in range(self.count):
                @pl.when(a >= 0)
                def _():
                    src = self.buf.at[a, y, j]
                    self.right(a, j, src).wait_recv()

                    @pl.when(z + 1 < links)
                    def _():
                        self.right(a, j, src).start()
                    self.across(a, j, y).start()

                @pl.when(b < links)
                def _():
                    src = self.buf.at[b, y, j]
                    self.left(b, j, src).wait_recv()

                    @pl.when(z > 0)
                    def _():
                        self.left(b, j, src).start()
                    self.across(b, j, y).start()

        def arrive(self, a):
            for j in range(self.count):
                self.across(a, j, 1 - y).wait_recv()

        def drain(self):
            def one(a, c):
                for j in range(self.count):
                    src = self.buf.at[a, y, j]

                    @pl.when((a <= z) & (z + 1 < links))
                    def _():
                        self.right(a, j, src).wait_send()

                    @pl.when((a >= z) & (z > 0))
                    def _():
                        self.left(a, j, src).wait_send()

                    @pl.when(a != z)
                    def _():
                        self.across(a, j, y).wait_send()
                return c
            lax.fori_loop(0, links, one, 0)

    qkv = Chain(w, wbuf, wz, wr, wl, wy, wys, subs)
    och = Chain(o, obuf, oz, orr, ol, oy, oys, osubs)

    def start_o(s):
        @pl.when((s == z) & (z + 1 < links))
        def _():
            och.start_right()

        @pl.when((s == links - 1 - z) & (z > 0))
        def _():
            och.start_left()

    @pl.when(z + 1 < links)
    def _():
        qkv.start_right()

    @pl.when(z > 0)
    def _():
        qkv.start_left()

    def tokens(a):
        return rdma(tok.at[2 * a + (1 - x)], ptok.at[a], ts.at[a], tr.at[a], dp=mate)

    def send_tokens(k, c):
        tokens((z + k) % links).start()
        return c

    lax.fori_loop(0, links, send_tokens, 0)
    start_o(0)

    slot = jnp.full(dmine.shape, dest_ref[0], jnp.int32)
    dmine[...] = slot
    dall[me] = slot

    def tell(k):
        peer = (me + k) % n
        return rdma(dmine, dall.at[me], des.at[peer], der.at[me], dp=peer)

    def send_slots(k, c):
        tell(k).start()
        return c

    lax.fori_loop(1, n, send_slots, 0)

    wbuf[z] = w[...]
    obuf[z] = o[...]
    acc[...] = jnp.zeros_like(acc)
    depth = tok.shape[2]

    def multiply(a):
        weight = wbuf[a].reshape(depth, wbuf.shape[-1])
        acc[0] += jnp.dot(tok[2 * a + x], weight, preferred_element_type=F32)
        acc[1] += jnp.dot(ptok[a], weight, preferred_element_type=F32)

    def step(s, c):
        qkv.forward(s)
        start_o(s)

        def side(k, c):
            a = jnp.where(k == 0, z - (s - 1), z + (s - 1))

            @pl.when((a >= 0) & (a < links) & ((k == 0) | (s > 1)))
            def _():
                @pl.when(s > 1)
                def _():
                    qkv.arrive(a)
                tokens(a).wait_recv()
                multiply(a)
            return c
        lax.fori_loop(0, 2, side, 0)
        return c

    lax.fori_loop(1, links + 1, step, 0)

    def partial(g):
        return rdma(psend.at[g], precv.at[g], ps.at[g], pr.at[g], dp=mate)

    for g in range(groups):
        psend[g] = acc[1, :, g * block:(g + 1) * block].astype(BF16)
        partial(g).start()

    if links > 1:
        och.forward(1)

    length = length_ref[0]
    cosine, sine = cos_ref[...], sin_ref[...]

    def rotate(u):
        return u * cosine + pltpu.roll(u, HD // 2, axis=1) * sine

    live = lax.broadcasted_iota(jnp.int32, (total, HD), 0) < length
    span = cflat.shape[0] // 2
    run = groups * half

    def regroup(kind):
        rows = pl.ds(pl.multiple_of(kind * span + t * run, half), run)
        return rdma(csend.at[kind], cflat.at[rows], cs.at[kind], cr.at[kind], tensor=1 - t)

    for g in range(groups):
        partial(g).wait_recv()
        lo = g * block + width
        keys = acc[0, :, lo:lo + HD] + precv[g, :, width:width + HD].astype(F32)
        values = acc[0, :, lo + HD:lo + 2 * HD] + precv[g, :, width + HD:].astype(F32)
        for kind, got in enumerate((rotate(keys), values)):
            kbuf[kind, g] = got.astype(BF16)
            kept = jnp.where(live, got, 0.0)
            first, second = kept[:half], kept[half:]
            mine = jnp.where(t == 0, first, second).astype(BF16)
            other = jnp.where(t == 0, second, first).astype(BF16)
            csend[kind, g * half:(g + 1) * half] = other
            start = pl.multiple_of(kind * span + t * run + g * half, half)
            cflat[pl.ds(start, half)] = mine
    for kind in range(2):
        regroup(kind).start()

    def rows_of(p):
        return pl.ds(pl.multiple_of(p * piece, piece), piece)

    def spread_to(k):
        peer = (me + k) % n
        return rdma(cflat.at[rows_of(peer)], spread.at[me], p1s.at[peer], p1r.at[me], dp=peer)

    for kind in range(2):
        other = pl.ds(pl.multiple_of(kind * span + (1 - t) * run, half), run)
        rdma(csend.at[kind], cflat.at[other], cs.at[kind], cr.at[kind], tensor=1 - t).wait_recv()

    def send_spread(k, c):
        spread_to(k).start()
        return c

    lax.fori_loop(1, n, send_spread, 0)
    spread[me] = cflat[rows_of(me)]

    row = lax.broadcasted_iota(jnp.int32, (total, total), 0)
    col = lax.broadcasted_iota(jnp.int32, (total, total), 1)
    allowed = (row >= col) & (col < length)

    def attended(g):
        return rdma(asend.at[g], arecv.at[g], as_.at[g], ar.at[g], dp=mate)

    for g in range(groups):
        keys, values = kbuf[0, g], kbuf[1, g]
        for h in range(group):
            lo = g * block + h * HD
            raw = acc[0, :, lo:lo + HD] + precv[g, :, h * HD:(h + 1) * HD].astype(F32)
            query = rotate(raw).astype(BF16)
            scores = lax.dot_general(
                query, keys, (((1,), (1,)), ((), ())), preferred_element_type=F32
            ) / math.sqrt(HD)
            scores = jnp.where(allowed, scores, -jnp.inf)
            peak = jnp.max(scores, axis=-1, keepdims=True)
            expo = jnp.exp(scores - peak)
            weights = (expo / jnp.sum(expo, axis=-1, keepdims=True)).astype(BF16)
            asend[g, :, h * HD:(h + 1) * HD] = jnp.dot(
                weights, values, preferred_element_type=F32).astype(BF16)
        attended(g).start()

    def rest(s, c):
        och.forward(s)
        return c

    lax.fori_loop(2, links, rest, 0)

    def wait_first(k, c):
        p = (me + k) % n
        rdma(dmine, dall.at[p], des.at[p], der.at[p], dp=p).wait_recv()
        rdma(cflat.at[rows_of(p)], spread.at[p], p1s.at[p], p1r.at[p], dp=p).wait_recv()
        return c

    lax.fori_loop(1, n, wait_first, 0)

    def hand(s):
        return rdma(going.at[s], final.at[me], p2s.at[s], p2r.at[me], dp=s)

    def route(k, c):
        s = (me + k) % n

        def add(p, value):
            mask = (dall[p][0:1, :] == s).astype(F32)
            return value + spread[p].astype(F32) * mask

        got = lax.fori_loop(0, n, add, jnp.zeros((piece, HD), F32)).astype(BF16)

        @pl.when(k > 0)
        def _():
            going[s] = got
            hand(s).start()

        @pl.when(k == 0)
        def _():
            final[me] = got
        return c

    lax.fori_loop(0, n, route, 0)

    def await_o(a, c):
        @pl.when(a != z)
        def _():
            och.arrive(a)
        return c

    lax.fori_loop(0, links, await_o, 0)
    for g in range(groups):
        attended(g).wait_recv()

    def project(a, ref):
        value = None
        for g in range(groups):
            weight = obuf[a].reshape(groups, width, obuf.shape[-1])[g]
            term = jnp.dot(ref[g], weight, preferred_element_type=F32)
            value = term if value is None else value + term
        return value

    def swap(i):
        return rdma(dsend.at[i], drecv.at[i], ds.at[i], dr.at[i], tensor=1 - t)

    def away(i, c):
        a = (1 - t) * homes + i
        dsend[i, 1] = project(a, arecv)
        dsend[i, 0] = project(a, asend)
        swap(i).start()
        return c

    lax.fori_loop(0, homes, away, 0)

    def give(i):
        return rdma(xsend.at[i], xrecv.at[i], xs.at[i], xr.at[i], dp=mate)

    def home(i, c):
        a = t * homes + i
        theirs, ours = project(a, arecv), project(a, asend)
        swap(i).wait_recv()
        xsend[i] = (theirs + drecv[i, 1]).astype(BF16)
        give(i).start()
        out[2 * i + x] = (ours + drecv[i, 0]).astype(BF16)
        return c

    lax.fori_loop(0, homes, home, 0)

    def last(k, c):
        p = (me + k) % n
        rdma(going.at[p], final.at[p], p2s.at[p], p2r.at[p], dp=p).wait_recv()
        return c

    lax.fori_loop(1, n, last, 0)
    cache[...] = final[...]

    def take(i, c):
        give(i).wait_recv()
        out[2 * i + (1 - x)] = xrecv[i]
        return c

    lax.fori_loop(0, homes, take, 0)

    qkv.drain()
    och.drain()

    def drain_tokens(a, c):
        tokens(a).wait_send()
        return c

    lax.fori_loop(0, links, drain_tokens, 0)
    for g in range(groups):
        partial(g).wait_send()
        attended(g).wait_send()
    for kind in range(2):
        regroup(kind).wait_send()

    def drain_peers(k, c):
        tell(k).wait_send()
        spread_to(k).wait_send()
        hand((me + k) % n).wait_send()
        return c

    lax.fori_loop(1, n, drain_peers, 0)

    def drain_homes(i, c):
        swap(i).wait_send()
        give(i).wait_send()
        return c

    lax.fori_loop(0, homes, drain_homes, 0)


def pieces_of(rows, columns):
    count = 2
    if rows % 32 or rows * columns * 2 < 262144:
        count = 1
    return count


def on_device(n, normed, q_weight, kv_weight, o_weight, lengths, destinations):
    total, model = normed.shape[1], normed.shape[2]
    rows, q_columns = q_weight.shape
    groups = kv_weight.shape[2] // HD
    group = q_columns // HD // groups
    width = group * HD
    parts = []
    for g in range(groups):
        parts.append(q_weight[:, g * width:(g + 1) * width])
        parts.append(kv_weight[:, 0, g * HD:(g + 1) * HD])
        parts.append(kv_weight[:, 1, g * HD:(g + 1) * HD])
    w = jnp.concatenate(parts, axis=1)
    columns = w.shape[1]
    subs = pieces_of(rows // 2, columns)
    w = w.reshape(2, subs, rows // 2 // subs, columns)
    o_rows, o_columns = o_weight.shape
    osubs = pieces_of(o_rows // 2, o_columns)
    o = o_weight.reshape(2, osubs, o_rows // 2 // osubs, o_columns)
    tok = normed[0].reshape(total, n, rows).transpose(1, 0, 2)
    cosine, sine = tables(total)
    links, homes = n // 2, n // 4
    block = width + 2 * HD
    half = total // 2
    cache_rows = 2 * 2 * groups * half
    piece = cache_rows // n
    dma = pltpu.SemaphoreType.DMA
    vmem = pltpu.VMEM
    space = pl.BlockSpec(memory_space=pltpu.VMEM)
    smem = pl.BlockSpec(memory_space=pltpu.SMEM)
    chain = lambda count: [dma((links, count))] * 5
    out, cache = pl.pallas_call(
        functools.partial(kernel, n, groups, group),
        out_shape=(
            jax.ShapeDtypeStruct((n // 2, total, o_columns), BF16),
            jax.ShapeDtypeStruct((n, piece, HD), BF16),
        ),
        in_specs=[smem, smem] + [space] * 5,
        out_specs=(space, space),
        scratch_shapes=[
            vmem((links,) + w.shape, BF16),
            vmem((links,) + o.shape, BF16),
            vmem((links, total, rows), BF16),
            vmem((2, total, columns), F32),
            vmem((groups, total, block), BF16),
            vmem((groups, total, block), BF16),
            vmem((groups, total, width), BF16),
            vmem((groups, total, width), BF16),
            vmem((homes, 2, total, o_columns), F32),
            vmem((homes, 2, total, o_columns), F32),
            vmem((homes, total, o_columns), BF16),
            vmem((homes, total, o_columns), BF16),
            vmem((2, groups * half, HD), BF16),
            vmem((cache_rows, HD), BF16),
            vmem((n, piece, HD), BF16),
            vmem((n, piece, HD), BF16),
            vmem((n, piece, HD), BF16),
            vmem((8, HD), jnp.int32),
            vmem((n, 8, HD), jnp.int32),
            vmem((2, groups, total, HD), BF16),
        ]
        + chain(subs) + chain(osubs)
        + [dma((links,))] * 2 + [dma((groups,))] * 4 + [dma((homes,))] * 4
        + [dma((2,))] * 2 + [dma((n,))] * 6,
        compiler_params=pltpu.CompilerParams(
            collective_id=0, has_side_effects=True, vmem_limit_bytes=60 * 1024 * 1024
        ),
    )(lengths, destinations, tok, w, o, cosine, sine)
    projected = out.transpose(1, 0, 2).reshape(1, total, -1)
    return projected, cache.reshape(1, 2, 2 * groups, half, HD)


def solution(mesh):
    placed = (
        P(("parts", "dp"), None, None),
        P("dp", "tensor"),
        P("dp", None, "tensor"),
        P("tensor", "dp"),
        P(("parts", "dp")),
        P(("parts", "dp")),
    )
    return jax.shard_map(
        functools.partial(on_device, mesh.shape["dp"]),
        mesh=mesh,
        in_specs=placed,
        out_specs=(
            P(("parts", "dp"), None, "tensor"),
            P(("parts", "dp"), None, None, "tensor", None),
        ),
        check_vma=False,
    )
```

```python
import functools
import math

import jax
import jax.numpy as jnp
from jax import lax
from jax.experimental import pallas as pl
from jax.experimental.pallas import tpu as pltpu
from jax.sharding import PartitionSpec as P

HD = 128
ROPE_BASE = 500000.0
MESH = pl.DeviceIdType.MESH
F32 = jnp.float32
BF16 = jnp.bfloat16


def tables(total):
    half = HD // 2
    steps = jnp.arange(half, dtype=F32) * (2.0 / HD)
    freq = jnp.power(jnp.float32(ROPE_BASE), -steps)
    angle = jnp.arange(total, dtype=F32)[:, None] * freq[None, :]
    cosine, sine = jnp.cos(angle), jnp.sin(angle)
    return (
        jnp.concatenate([cosine, cosine], axis=1),
        jnp.concatenate([-sine, sine], axis=1),
    )


def rdma(src, dst, send, recv, **device):
    return pltpu.make_async_remote_copy(
        src_ref=src, dst_ref=dst, send_sem=send, recv_sem=recv,
        device_id=device, device_id_type=MESH,
    )


def kernel(n, groups, group, length_ref, dest_ref, tok, q, kv, o, cos_ref, sin_ref,
           out, cache,
           wbuf, obuf, ptok, acc, psend, precv, asend, arecv, dsend, drecv,
           xsend, xrecv, csend, cflat, spread, going, final, dmine, dall, kbuf,
           wz, wr, wl, wy, wys, oz, orr, ol, oy, oys,
           ts, tr, ps, pr, as_, ar, ds, dr, xs, xr, cs, cr,
           des, der, p1s, p1r, p2s, p2r):
    me = lax.axis_index("dp")
    y = lax.axis_index("parts")
    t = lax.axis_index("tensor")
    z = me // 2
    x = me % 2
    links = n // 2
    mate = z * 2 + (1 - x)
    total = cos_ref.shape[0]
    depth, ocols = q.shape[0], o.shape[-1]
    subs, osubs = wbuf.shape[3], o.shape[1]
    flat = depth % HD == 0
    width = group * HD
    block = width + 2 * HD
    half = total // 2
    piece = spread.shape[1]
    homes = links // 2

    for g in range(groups):
        shape = wbuf.shape[2:5]
        wbuf[g, z, :, :, :, :width] = q[:, g * width:(g + 1) * width].reshape(shape + (width,))
        wbuf[g, z, :, :, :, width:] = kv[g].reshape(shape + (2 * HD,))

    barrier = pltpu.get_barrier_semaphore()

    def greet(k, c):
        pl.semaphore_signal(
            barrier, inc=1, device_id={"dp": (me + k) % n}, device_id_type=MESH)
        return c

    lax.fori_loop(1, n, greet, 0)
    pl.semaphore_signal(barrier, inc=1, device_id={"tensor": 1 - t}, device_id_type=MESH)
    pl.semaphore_signal(barrier, inc=1, device_id={"parts": 1 - y}, device_id_type=MESH)
    pl.semaphore_wait(barrier, n + 1)

    class Chain:
        def __init__(self, own, buf, zr, sr, sl, yr, ys, count):
            self.own, self.buf, self.count = own, buf, count
            self.zr, self.sr, self.sl, self.yr, self.ys = zr, sr, sl, yr, ys

        def right(self, a, j, src):
            return rdma(src, self.buf.at[a, y, j], self.sr.at[a, j], self.zr.at[a, j], dp=me + 2)

        def left(self, a, j, src):
            return rdma(src, self.buf.at[a, y, j], self.sl.at[a, j], self.zr.at[a, j], dp=me - 2)

        def across(self, a, j, side):
            part = self.buf.at[a, side, j]
            return rdma(part, part, self.ys.at[a, j], self.yr.at[a, j], parts=1 - y)

        def start_right(self):
            for j in range(self.count):
                self.right(z, j, self.own.at[y, j]).start()

        def start_left(self):
            for j in range(self.count):
                self.left(z, j, self.own.at[y, j]).start()

        def forward(self, s):
            a, b = z - s, z + s
            for j in range(self.count):
                @pl.when(a >= 0)
                def _():
                    src = self.buf.at[a, y, j]
                    self.right(a, j, src).wait_recv()

                    @pl.when(z + 1 < links)
                    def _():
                        self.right(a, j, src).start()
                    self.across(a, j, y).start()

                @pl.when(b < links)
                def _():
                    src = self.buf.at[b, y, j]
                    self.left(b, j, src).wait_recv()

                    @pl.when(z > 0)
                    def _():
                        self.left(b, j, src).start()
                    self.across(b, j, y).start()

        def arrive(self, a):
            for j in range(self.count):
                self.across(a, j, 1 - y).wait_recv()

        def drain(self):
            def one(a, c):
                for j in range(self.count):
                    src = self.buf.at[a, y, j]

                    @pl.when((a <= z) & (z + 1 < links))
                    def _():
                        self.right(a, j, src).wait_send()

                    @pl.when((a >= z) & (z > 0))
                    def _():
                        self.left(a, j, src).wait_send()

                    @pl.when(a != z)
                    def _():
                        self.across(a, j, y).wait_send()
                return c
            lax.fori_loop(0, links, one, 0)

    chains = [
        Chain(wbuf.at[g, z], wbuf.at[g], *(sem.at[g] for sem in (wz, wr, wl, wy, wys)), subs)
        for g in range(groups)
    ]
    och = Chain(o, obuf, oz, orr, ol, oy, oys, osubs)

    chains.append(och)

    def follow(g, s):
        @pl.when((s == z) & (z + 1 < links))
        def _():
            chains[g + 1].start_right()

        @pl.when((s == links - 1 - z) & (z > 0))
        def _():
            chains[g + 1].start_left()

    @pl.when(z + 1 < links)
    def _():
        chains[0].start_right()

    @pl.when(z > 0)
    def _():
        chains[0].start_left()

    def columns_of(d):
        if flat:
            return tok.at[:, pl.ds(pl.multiple_of(d * depth, HD), depth)]
        return tok.at[d]

    def tokens(a):
        return rdma(columns_of(2 * a + (1 - x)), ptok.at[a], ts.at[a], tr.at[a], dp=mate)

    def send_tokens(k, c):
        tokens((z + k) % links).start()
        return c

    lax.fori_loop(0, links, send_tokens, 0)
    slot = jnp.full(dmine.shape, dest_ref[0], jnp.int32)
    dmine[...] = slot
    dall[me] = slot

    def tell(k):
        peer = (me + k) % n
        return rdma(dmine, dall.at[me], des.at[peer], der.at[me], dp=peer)

    def send_slots(k, c):
        tell(k).start()
        return c

    lax.fori_loop(1, n, send_slots, 0)

    obuf[z] = o[...]
    acc[...] = jnp.zeros_like(acc)

    def multiply(g, a):
        weight = wbuf[g, a].reshape(depth, block)
        acc[g, 0] += jnp.dot(columns_of(2 * a + x)[...], weight, preferred_element_type=F32)
        acc[g, 1] += jnp.dot(ptok[a], weight, preferred_element_type=F32)

    def partial(g):
        return rdma(psend.at[g], precv.at[g], ps.at[g], pr.at[g], dp=mate)

    for g in range(groups):
        follow(g, 0)

        def step(s, c, g=g):
            chains[g].forward(s)
            follow(g, s)

            def side(k, c):
                a = jnp.where(k == 0, z - (s - 1), z + (s - 1))

                @pl.when((a >= 0) & (a < links) & ((k == 0) | (s > 1)))
                def _():
                    @pl.when(s > 1)
                    def _():
                        chains[g].arrive(a)
                    if g == 0:
                        tokens(a).wait_recv()
                    multiply(g, a)
                return c
            lax.fori_loop(0, 2, side, 0)
            return c

        lax.fori_loop(1, links + 1, step, 0)
        psend[g] = acc[g, 1].astype(BF16)
        partial(g).start()

    if links > 1:
        och.forward(1)

    length = length_ref[0]
    cosine, sine = cos_ref[...], sin_ref[...]

    def rotate(u):
        return u * cosine + pltpu.roll(u, HD // 2, axis=1) * sine

    live = lax.broadcasted_iota(jnp.int32, (total, HD), 0) < length
    span = cflat.shape[0] // 2
    run = groups * half

    def regroup(kind):
        rows = pl.ds(pl.multiple_of(kind * span + t * run, half), run)
        return rdma(csend.at[kind], cflat.at[rows], cs.at[kind], cr.at[kind], tensor=1 - t)

    row = lax.broadcasted_iota(jnp.int32, (total, total), 0)
    col = lax.broadcasted_iota(jnp.int32, (total, total), 1)
    allowed = (row >= col) & (col < length)

    def attended(g):
        return rdma(asend.at[g], arecv.at[g], as_.at[g], ar.at[g], dp=mate)

    for g in range(groups):
        partial(g).wait_recv()
        keys = acc[g, 0, :, width:width + HD] + precv[g, :, width:width + HD].astype(F32)
        values = acc[g, 0, :, width + HD:] + precv[g, :, width + HD:].astype(F32)
        for kind, got in enumerate((rotate(keys), values)):
            kbuf[kind, g] = got.astype(BF16)
            kept = jnp.where(live, got, 0.0)
            first, second = kept[:half], kept[half:]
            mine = jnp.where(t == 0, first, second).astype(BF16)
            other = jnp.where(t == 0, second, first).astype(BF16)
            csend[kind, g * half:(g + 1) * half] = other
            start = pl.multiple_of(kind * span + t * run + g * half, half)
            cflat[pl.ds(start, half)] = mine
        if g == groups - 1:
            for kind in range(2):
                regroup(kind).start()
        keys, values = kbuf[0, g], kbuf[1, g]
        for h in range(group):
            lo = h * HD
            raw = acc[g, 0, :, lo:lo + HD] + precv[g, :, lo:lo + HD].astype(F32)
            query = rotate(raw).astype(BF16)
            scores = lax.dot_general(
                query, keys, (((1,), (1,)), ((), ())), preferred_element_type=F32
            ) / math.sqrt(HD)
            scores = jnp.where(allowed, scores, -jnp.inf)
            peak = jnp.max(scores, axis=-1, keepdims=True)
            expo = jnp.exp(scores - peak)
            weights = (expo / jnp.sum(expo, axis=-1, keepdims=True)).astype(BF16)
            asend[g, :, lo:lo + HD] = jnp.dot(
                weights, values, preferred_element_type=F32).astype(BF16)
        attended(g).start()

    def rows_of(p):
        return pl.ds(pl.multiple_of(p * piece, piece), piece)

    def spread_to(k):
        peer = (me + k) % n
        return rdma(cflat.at[rows_of(peer)], spread.at[me], p1s.at[peer], p1r.at[me], dp=peer)

    for kind in range(2):
        other = pl.ds(pl.multiple_of(kind * span + (1 - t) * run, half), run)
        rdma(csend.at[kind], cflat.at[other], cs.at[kind], cr.at[kind], tensor=1 - t).wait_recv()

    def send_spread(k, c):
        spread_to(k).start()
        return c

    lax.fori_loop(1, n, send_spread, 0)
    spread[me] = cflat[rows_of(me)]

    def rest(s, c):
        och.forward(s)
        return c

    lax.fori_loop(2, links, rest, 0)

    def await_o(a, c):
        @pl.when(a != z)
        def _():
            och.arrive(a)
        return c

    lax.fori_loop(0, links, await_o, 0)
    def project(a, ref):
        value = None
        for g in range(groups):
            weight = obuf[a].reshape(groups, width, ocols)[g]
            term = jnp.dot(ref[g], weight, preferred_element_type=F32)
            value = term if value is None else value + term
        return value

    def swap(i, side):
        return rdma(dsend.at[i, side], drecv.at[i, side], ds.at[i, side], dr.at[i, side],
                    tensor=1 - t)

    def away(side, ref):
        def one(i, c):
            dsend[i, side] = project((1 - t) * homes + i, ref)
            swap(i, side).start()
            return c
        lax.fori_loop(0, homes, one, 0)

    away(0, asend)
    for g in range(groups):
        attended(g).wait_recv()
    away(1, arecv)

    def give(i):
        return rdma(xsend.at[i], xrecv.at[i], xs.at[i], xr.at[i], dp=mate)

    def theirs(i, c):
        value = project(t * homes + i, arecv)
        swap(i, 1).wait_recv()
        xsend[i] = (value + drecv[i, 1]).astype(BF16)
        give(i).start()
        return c

    lax.fori_loop(0, homes, theirs, 0)

    def wait_first(k, c):
        p = (me + k) % n
        rdma(dmine, dall.at[p], des.at[p], der.at[p], dp=p).wait_recv()
        rdma(cflat.at[rows_of(p)], spread.at[p], p1s.at[p], p1r.at[p], dp=p).wait_recv()
        return c

    lax.fori_loop(1, n, wait_first, 0)

    def hand(s):
        return rdma(going.at[s], final.at[me], p2s.at[s], p2r.at[me], dp=s)

    def route(k, c):
        s = (me + k) % n

        def add(p, value):
            mask = (dall[p][0:1, :] == s).astype(F32)
            return value + spread[p].astype(F32) * mask

        got = lax.fori_loop(0, n, add, jnp.zeros((piece, HD), F32)).astype(BF16)

        @pl.when(k > 0)
        def _():
            going[s] = got
            hand(s).start()

        @pl.when(k == 0)
        def _():
            final[me] = got
        return c

    lax.fori_loop(0, n, route, 0)

    def put(d, value):
        if ocols % HD == 0:
            out[:, pl.ds(pl.multiple_of(d * ocols, HD), ocols)] = value
        else:
            out[d] = value

    def ours(i, c):
        value = project(t * homes + i, asend)
        swap(i, 0).wait_recv()
        put(2 * i + x, (value + drecv[i, 0]).astype(BF16))
        return c

    lax.fori_loop(0, homes, ours, 0)

    def last(k, c):
        p = (me + k) % n
        rdma(going.at[p], final.at[p], p2s.at[p], p2r.at[p], dp=p).wait_recv()
        return c

    lax.fori_loop(1, n, last, 0)
    cache[...] = final[...]

    def take(i, c):
        give(i).wait_recv()
        put(2 * i + (1 - x), xrecv[i])
        return c

    lax.fori_loop(0, homes, take, 0)

    for one in chains:
        one.drain()

    def drain_tokens(a, c):
        tokens(a).wait_send()
        return c

    lax.fori_loop(0, links, drain_tokens, 0)
    for g in range(groups):
        partial(g).wait_send()
        attended(g).wait_send()
    for kind in range(2):
        regroup(kind).wait_send()

    def drain_peers(k, c):
        tell(k).wait_send()
        spread_to(k).wait_send()
        hand((me + k) % n).wait_send()
        return c

    lax.fori_loop(1, n, drain_peers, 0)

    def drain_homes(i, c):
        swap(i, 0).wait_send()
        swap(i, 1).wait_send()
        give(i).wait_send()
        return c

    lax.fori_loop(0, homes, drain_homes, 0)


def pieces_of(rows, columns):
    count = 2
    if rows % 32 or rows * columns * 2 < 262144:
        count = 1
    return count


def on_device(n, normed, q_weight, kv_weight, o_weight, lengths, destinations):
    total, model = normed.shape[1], normed.shape[2]
    rows, q_columns = q_weight.shape
    groups = kv_weight.shape[2] // HD
    group = q_columns // HD // groups
    width = group * HD
    block = width + 2 * HD
    kv = kv_weight.reshape(rows, 2, groups, HD).transpose(2, 0, 1, 3)
    kv = kv.reshape(groups, rows, 2 * HD)
    subs = pieces_of(rows // 2, block)
    shard = (2, subs, rows // 2 // subs, block)
    o_rows, o_columns = o_weight.shape
    osubs = pieces_of(o_rows // 2, o_columns)
    o = o_weight.reshape(2, osubs, o_rows // 2 // osubs, o_columns)
    tok = normed[0]
    if rows % HD:
        tok = tok.reshape(total, n, rows).transpose(1, 0, 2)
    cosine, sine = tables(total)
    links, homes = n // 2, n // 4
    half = total // 2
    cache_rows = 2 * 2 * groups * half
    piece = cache_rows // n
    dma = pltpu.SemaphoreType.DMA
    vmem = pltpu.VMEM
    space = pl.BlockSpec(memory_space=pltpu.VMEM)
    smem = pl.BlockSpec(memory_space=pltpu.SMEM)
    straight = o_columns % HD == 0
    shape = (n // 2, total, o_columns)
    if straight:
        shape = (total, n // 2 * o_columns)
    out, cache = pl.pallas_call(
        functools.partial(kernel, n, groups, group),
        out_shape=(
            jax.ShapeDtypeStruct(shape, BF16),
            jax.ShapeDtypeStruct((n, piece, HD), BF16),
        ),
        in_specs=[smem, smem] + [space] * 6,
        out_specs=(space, space),
        scratch_shapes=[
            vmem((groups, links) + shard, BF16),
            vmem((links,) + o.shape, BF16),
            vmem((links, total, rows), BF16),
            vmem((groups, 2, total, block), F32),
            vmem((groups, total, block), BF16),
            vmem((groups, total, block), BF16),
            vmem((groups, total, width), BF16),
            vmem((groups, total, width), BF16),
            vmem((homes, 2, total, o_columns), F32),
            vmem((homes, 2, total, o_columns), F32),
            vmem((homes, total, o_columns), BF16),
            vmem((homes, total, o_columns), BF16),
            vmem((2, groups * half, HD), BF16),
            vmem((cache_rows, HD), BF16),
            vmem((n, piece, HD), BF16),
            vmem((n, piece, HD), BF16),
            vmem((n, piece, HD), BF16),
            vmem((8, HD), jnp.int32),
            vmem((n, 8, HD), jnp.int32),
            vmem((2, groups, total, HD), BF16),
        ]
        + [dma((groups, links, subs))] * 5 + [dma((links, osubs))] * 5
        + [dma((links,))] * 2 + [dma((groups,))] * 4 + [dma((homes, 2))] * 2 + [dma((homes,))] * 2
        + [dma((2,))] * 2 + [dma((n,))] * 6,
        compiler_params=pltpu.CompilerParams(
            collective_id=0, has_side_effects=True, vmem_limit_bytes=60 * 1024 * 1024
        ),
    )(lengths, destinations, tok, q_weight, kv, o, cosine, sine)
    if not straight:
        out = out.transpose(1, 0, 2)
    projected = out.reshape(1, total, -1)
    return projected, cache.reshape(1, 2, 2 * groups, half, HD)


def solution(mesh):
    placed = (
        P(("parts", "dp"), None, None),
        P("dp", "tensor"),
        P("dp", None, "tensor"),
        P("tensor", "dp"),
        P(("parts", "dp")),
        P(("parts", "dp")),
    )
    return jax.shard_map(
        functools.partial(on_device, mesh.shape["dp"]),
        mesh=mesh,
        in_specs=placed,
        out_specs=(
            P(("parts", "dp"), None, "tensor"),
            P(("parts", "dp"), None, None, "tensor", None),
        ),
        check_vma=False,
    )
```

```python
import functools
import math

import jax
import jax.numpy as jnp
from jax import lax
from jax.experimental import pallas as pl
from jax.experimental.pallas import tpu as pltpu
from jax.sharding import PartitionSpec as P

HD = 128
ROPE_BASE = 500000.0
MESH = pl.DeviceIdType.MESH
F32 = jnp.float32
BF16 = jnp.bfloat16


def tables(total):
    half = HD // 2
    steps = jnp.arange(half, dtype=F32) * (2.0 / HD)
    freq = jnp.power(jnp.float32(ROPE_BASE), -steps)
    angle = jnp.arange(total, dtype=F32)[:, None] * freq[None, :]
    cosine, sine = jnp.cos(angle), jnp.sin(angle)
    return (
        jnp.concatenate([cosine, cosine], axis=1),
        jnp.concatenate([-sine, sine], axis=1),
    )


def rdma(src, dst, send, recv, **device):
    return pltpu.make_async_remote_copy(
        src_ref=src, dst_ref=dst, send_sem=send, recv_sem=recv,
        device_id=device, device_id_type=MESH,
    )


def kernel(n, groups, group, length_ref, dest_ref, tok, q, kv, o, cos_ref, sin_ref,
           out, cache,
           wbuf, obuf, ptok, acc, psend, precv, asend, arecv, dsend, drecv,
           xsend, xrecv, csend, cflat, spread, going, final, dmine, dall, kbuf,
           wz, wr, wl, wy, wys, oz, orr, ol, oy, oys,
           ts, tr, ps, pr, as_, ar, ds, dr, xs, xr, cs, cr,
           des, der, p1s, p1r, p2s, p2r):
    me = lax.axis_index("dp")
    y = lax.axis_index("parts")
    t = lax.axis_index("tensor")
    z = me // 2
    x = me % 2
    links = n // 2
    mate = z * 2 + (1 - x)
    total = cos_ref.shape[0]
    depth, ocols = q.shape[0], o.shape[-1]
    subs, osubs = wbuf.shape[3], o.shape[1]
    flat = depth % HD == 0
    width = group * HD
    block = width + 2 * HD
    half = total // 2
    piece = spread.shape[1]
    homes = links // 2

    for g in range(groups):
        shape = wbuf.shape[2:5]
        wbuf[g, z, :, :, :, :width] = q[:, g * width:(g + 1) * width].reshape(shape + (width,))
        wbuf[g, z, :, :, :, width:] = kv[g].reshape(shape + (2 * HD,))

    barrier = pltpu.get_barrier_semaphore()

    def greet(k, c):
        pl.semaphore_signal(
            barrier, inc=1, device_id={"dp": (me + k) % n}, device_id_type=MESH)
        return c

    lax.fori_loop(1, n, greet, 0)
    pl.semaphore_signal(barrier, inc=1, device_id={"tensor": 1 - t}, device_id_type=MESH)
    pl.semaphore_signal(barrier, inc=1, device_id={"parts": 1 - y}, device_id_type=MESH)
    pl.semaphore_wait(barrier, n + 1)

    class Chain:
        def __init__(self, own, buf, zr, sr, sl, yr, ys, count):
            self.own, self.buf, self.count = own, buf, count
            self.zr, self.sr, self.sl, self.yr, self.ys = zr, sr, sl, yr, ys

        def right(self, a, j, src):
            return rdma(src, self.buf.at[a, y, j], self.sr.at[a, j], self.zr.at[a, j], dp=me + 2)

        def left(self, a, j, src):
            return rdma(src, self.buf.at[a, y, j], self.sl.at[a, j], self.zr.at[a, j], dp=me - 2)

        def across(self, a, j, side):
            part = self.buf.at[a, side, j]
            return rdma(part, part, self.ys.at[a, j], self.yr.at[a, j], parts=1 - y)

        def start_right(self):
            for j in range(self.count):
                self.right(z, j, self.own.at[y, j]).start()

        def start_left(self):
            for j in range(self.count):
                self.left(z, j, self.own.at[y, j]).start()

        def forward(self, s):
            a, b = z - s, z + s
            for j in range(self.count):
                @pl.when(a >= 0)
                def _():
                    src = self.buf.at[a, y, j]
                    self.right(a, j, src).wait_recv()

                    @pl.when(z + 1 < links)
                    def _():
                        self.right(a, j, src).start()
                    self.across(a, j, y).start()

                @pl.when(b < links)
                def _():
                    src = self.buf.at[b, y, j]
                    self.left(b, j, src).wait_recv()

                    @pl.when(z > 0)
                    def _():
                        self.left(b, j, src).start()
                    self.across(b, j, y).start()

        def arrive(self, a):
            for j in range(self.count):
                self.across(a, j, 1 - y).wait_recv()

        def drain(self):
            def one(a, c):
                for j in range(self.count):
                    src = self.buf.at[a, y, j]

                    @pl.when((a <= z) & (z + 1 < links))
                    def _():
                        self.right(a, j, src).wait_send()

                    @pl.when((a >= z) & (z > 0))
                    def _():
                        self.left(a, j, src).wait_send()

                    @pl.when(a != z)
                    def _():
                        self.across(a, j, y).wait_send()
                return c
            lax.fori_loop(0, links, one, 0)

    chains = [
        Chain(wbuf.at[g, z], wbuf.at[g], *(sem.at[g] for sem in (wz, wr, wl, wy, wys)), subs)
        for g in range(groups)
    ]
    och = Chain(o, obuf, oz, orr, ol, oy, oys, osubs)

    chains.append(och)

    def follow(g, s):
        @pl.when((s == z) & (z + 1 < links))
        def _():
            chains[g + 1].start_right()

        @pl.when((s == links - 1 - z) & (z > 0))
        def _():
            chains[g + 1].start_left()

    @pl.when(z + 1 < links)
    def _():
        chains[0].start_right()

    @pl.when(z > 0)
    def _():
        chains[0].start_left()

    def columns_of(d):
        if flat:
            return tok.at[:, pl.ds(pl.multiple_of(d * depth, HD), depth)]
        return tok.at[d]

    def tokens(a):
        return rdma(columns_of(2 * a + (1 - x)), ptok.at[a], ts.at[a], tr.at[a], dp=mate)

    def send_tokens(k, c):
        tokens((z + k) % links).start()
        return c

    lax.fori_loop(0, links, send_tokens, 0)
    slot = jnp.full(dmine.shape, dest_ref[0], jnp.int32)
    dmine[...] = slot
    dall[me] = slot

    def tell(k):
        peer = (me + k) % n
        return rdma(dmine, dall.at[me], des.at[peer], der.at[me], dp=peer)

    def send_slots(k, c):
        tell(k).start()
        return c

    lax.fori_loop(1, n, send_slots, 0)

    obuf[z] = o[...]
    acc[...] = jnp.zeros_like(acc)

    def multiply(g, a):
        weight = wbuf[g, a].reshape(depth, block)
        acc[g, 0] += jnp.dot(columns_of(2 * a + x)[...], weight, preferred_element_type=F32)
        acc[g, 1] += jnp.dot(ptok[a], weight, preferred_element_type=F32)

    def partial(g):
        return rdma(psend.at[g], precv.at[g], ps.at[g], pr.at[g], dp=mate)

    for g in range(groups):
        follow(g, 0)

        def step(s, c, g=g):
            chains[g].forward(s)
            follow(g, s)

            def side(k, c):
                a = jnp.where(k == 0, z - (s - 1), z + (s - 1))

                @pl.when((a >= 0) & (a < links) & ((k == 0) | (s > 1)))
                def _():
                    @pl.when(s > 1)
                    def _():
                        chains[g].arrive(a)
                    if g == 0:
                        tokens(a).wait_recv()
                    multiply(g, a)
                return c
            lax.fori_loop(0, 2, side, 0)
            return c

        lax.fori_loop(1, links + 1, step, 0)
        psend[g] = acc[g, 1].astype(BF16)
        partial(g).start()

    if links > 1:
        och.forward(1)

    length = length_ref[0]
    cosine, sine = cos_ref[...], sin_ref[...]

    def rotate(u):
        return u * cosine + pltpu.roll(u, HD // 2, axis=1) * sine

    live = lax.broadcasted_iota(jnp.int32, (total, HD), 0) < length
    span = cflat.shape[0] // 2
    run = groups * half

    def regroup(kind):
        rows = pl.ds(pl.multiple_of(kind * span + t * run, half), run)
        return rdma(csend.at[kind], cflat.at[rows], cs.at[kind], cr.at[kind], tensor=1 - t)

    row = lax.broadcasted_iota(jnp.int32, (total, total), 0)
    col = lax.broadcasted_iota(jnp.int32, (total, total), 1)
    allowed = (row >= col) & (col < length)

    def attended(g):
        return rdma(asend.at[g], arecv.at[g], as_.at[g], ar.at[g], dp=mate)

    for g in range(groups):
        partial(g).wait_recv()
        keys = acc[g, 0, :, width:width + HD] + precv[g, :, width:width + HD].astype(F32)
        values = acc[g, 0, :, width + HD:] + precv[g, :, width + HD:].astype(F32)
        for kind, got in enumerate((rotate(keys), values)):
            kbuf[kind, g] = got.astype(BF16)
            kept = jnp.where(live, got, 0.0)
            first, second = kept[:half], kept[half:]
            mine = jnp.where(t == 0, first, second).astype(BF16)
            other = jnp.where(t == 0, second, first).astype(BF16)
            csend[kind, g * half:(g + 1) * half] = other
            start = pl.multiple_of(kind * span + t * run + g * half, half)
            cflat[pl.ds(start, half)] = mine
        if g == groups - 1:
            for kind in range(2):
                regroup(kind).start()
        keys, values = kbuf[0, g], kbuf[1, g]
        for h in range(group):
            lo = h * HD
            raw = acc[g, 0, :, lo:lo + HD] + precv[g, :, lo:lo + HD].astype(F32)
            query = rotate(raw).astype(BF16)
            scores = lax.dot_general(
                query, keys, (((1,), (1,)), ((), ())), preferred_element_type=F32
            ) / math.sqrt(HD)
            scores = jnp.where(allowed, scores, -jnp.inf)
            peak = jnp.max(scores, axis=-1, keepdims=True)
            expo = jnp.exp(scores - peak)
            weights = (expo / jnp.sum(expo, axis=-1, keepdims=True)).astype(BF16)
            asend[g, :, lo:lo + HD] = jnp.dot(
                weights, values, preferred_element_type=F32).astype(BF16)
        attended(g).start()

    def rows_of(p):
        return pl.ds(pl.multiple_of(p * piece, piece), piece)

    def spread_to(k):
        peer = (me + k) % n
        return rdma(cflat.at[rows_of(peer)], spread.at[me], p1s.at[peer], p1r.at[me], dp=peer)

    for kind in range(2):
        other = pl.ds(pl.multiple_of(kind * span + (1 - t) * run, half), run)
        rdma(csend.at[kind], cflat.at[other], cs.at[kind], cr.at[kind], tensor=1 - t).wait_recv()

    def send_spread(k, c):
        spread_to(k).start()
        return c

    lax.fori_loop(1, n, send_spread, 0)
    spread[me] = cflat[rows_of(me)]

    def rest(s, c):
        och.forward(s)
        return c

    lax.fori_loop(2, links - homes + 1, rest, 0)

    def project(a, ref):
        value = None
        for g in range(groups):
            weight = obuf[a].reshape(groups, width, ocols)[g]
            term = jnp.dot(ref[g], weight, preferred_element_type=F32)
            value = term if value is None else value + term
        return value

    def swap(i, side):
        return rdma(dsend.at[i, side], drecv.at[i, side], ds.at[i, side], dr.at[i, side],
                    tensor=1 - t)

    def give(i):
        return rdma(xsend.at[i], xrecv.at[i], xs.at[i], xr.at[i], dp=mate)

    def await_o(a):
        @pl.when(a != z)
        def _():
            och.arrive(a)

    for g in range(groups):
        attended(g).wait_recv()

    def blocks(k, c):
        @pl.when(k > 0)
        def _():
            och.forward(links - homes + k)
        i = jnp.where(z >= homes, homes - 1 - k, k)
        far, near = (1 - t) * homes + i, t * homes + i
        await_o(far)
        dsend[i, 1] = project(far, arecv)
        swap(i, 1).start()
        await_o(near)
        value = project(near, arecv)
        swap(i, 1).wait_recv()
        xsend[i] = (value + drecv[i, 1]).astype(BF16)
        give(i).start()
        dsend[i, 0] = project(far, asend)
        swap(i, 0).start()
        return c

    lax.fori_loop(0, homes, blocks, 0)

    def wait_first(k, c):
        p = (me + k) % n
        rdma(dmine, dall.at[p], des.at[p], der.at[p], dp=p).wait_recv()
        rdma(cflat.at[rows_of(p)], spread.at[p], p1s.at[p], p1r.at[p], dp=p).wait_recv()
        return c

    lax.fori_loop(1, n, wait_first, 0)

    def hand(s):
        return rdma(going.at[s], final.at[me], p2s.at[s], p2r.at[me], dp=s)

    def route(k, c):
        s = (me + k) % n

        def add(p, value):
            mask = (dall[p][0:1, :] == s).astype(F32)
            return value + spread[p].astype(F32) * mask

        got = lax.fori_loop(0, n, add, jnp.zeros((piece, HD), F32)).astype(BF16)

        @pl.when(k > 0)
        def _():
            going[s] = got
            hand(s).start()

        @pl.when(k == 0)
        def _():
            final[me] = got
        return c

    lax.fori_loop(0, n, route, 0)

    def put(d, value):
        if ocols % HD == 0:
            out[:, pl.ds(pl.multiple_of(d * ocols, HD), ocols)] = value
        else:
            out[d] = value

    def ours(i, c):
        value = project(t * homes + i, asend)
        swap(i, 0).wait_recv()
        put(2 * i + x, (value + drecv[i, 0]).astype(BF16))
        return c

    lax.fori_loop(0, homes, ours, 0)

    def last(k, c):
        p = (me + k) % n
        rdma(going.at[p], final.at[p], p2s.at[p], p2r.at[p], dp=p).wait_recv()
        return c

    lax.fori_loop(1, n, last, 0)
    cache[...] = final[...]

    def take(i, c):
        give(i).wait_recv()
        put(2 * i + (1 - x), xrecv[i])
        return c

    lax.fori_loop(0, homes, take, 0)

    for one in chains:
        one.drain()

    def drain_tokens(a, c):
        tokens(a).wait_send()
        return c

    lax.fori_loop(0, links, drain_tokens, 0)
    for g in range(groups):
        partial(g).wait_send()
        attended(g).wait_send()
    for kind in range(2):
        regroup(kind).wait_send()

    def drain_peers(k, c):
        tell(k).wait_send()
        spread_to(k).wait_send()
        hand((me + k) % n).wait_send()
        return c

    lax.fori_loop(1, n, drain_peers, 0)

    def drain_homes(i, c):
        swap(i, 0).wait_send()
        swap(i, 1).wait_send()
        give(i).wait_send()
        return c

    lax.fori_loop(0, homes, drain_homes, 0)


def pieces_of(rows, columns):
    count = 2
    if rows % 32 or rows * columns * 2 < 262144:
        count = 1
    return count


def on_device(n, normed, q_weight, kv_weight, o_weight, lengths, destinations):
    total, model = normed.shape[1], normed.shape[2]
    rows, q_columns = q_weight.shape
    groups = kv_weight.shape[2] // HD
    group = q_columns // HD // groups
    width = group * HD
    block = width + 2 * HD
    kv = kv_weight.reshape(rows, 2, groups, HD).transpose(2, 0, 1, 3)
    kv = kv.reshape(groups, rows, 2 * HD)
    subs = pieces_of(rows // 2, block)
    shard = (2, subs, rows // 2 // subs, block)
    o_rows, o_columns = o_weight.shape
    osubs = pieces_of(o_rows // 2, o_columns)
    o = o_weight.reshape(2, osubs, o_rows // 2 // osubs, o_columns)
    tok = normed[0]
    if rows % HD:
        tok = tok.reshape(total, n, rows).transpose(1, 0, 2)
    cosine, sine = tables(total)
    links, homes = n // 2, n // 4
    half = total // 2
    cache_rows = 2 * 2 * groups * half
    piece = cache_rows // n
    dma = pltpu.SemaphoreType.DMA
    vmem = pltpu.VMEM
    space = pl.BlockSpec(memory_space=pltpu.VMEM)
    smem = pl.BlockSpec(memory_space=pltpu.SMEM)
    straight = o_columns % HD == 0
    shape = (n // 2, total, o_columns)
    if straight:
        shape = (total, n // 2 * o_columns)
    out, cache = pl.pallas_call(
        functools.partial(kernel, n, groups, group),
        out_shape=(
            jax.ShapeDtypeStruct(shape, BF16),
            jax.ShapeDtypeStruct((n, piece, HD), BF16),
        ),
        in_specs=[smem, smem] + [space] * 6,
        out_specs=(space, space),
        scratch_shapes=[
            vmem((groups, links) + shard, BF16),
            vmem((links,) + o.shape, BF16),
            vmem((links, total, rows), BF16),
            vmem((groups, 2, total, block), F32),
            vmem((groups, total, block), BF16),
            vmem((groups, total, block), BF16),
            vmem((groups, total, width), BF16),
            vmem((groups, total, width), BF16),
            vmem((homes, 2, total, o_columns), F32),
            vmem((homes, 2, total, o_columns), F32),
            vmem((homes, total, o_columns), BF16),
            vmem((homes, total, o_columns), BF16),
            vmem((2, groups * half, HD), BF16),
            vmem((cache_rows, HD), BF16),
            vmem((n, piece, HD), BF16),
            vmem((n, piece, HD), BF16),
            vmem((n, piece, HD), BF16),
            vmem((8, HD), jnp.int32),
            vmem((n, 8, HD), jnp.int32),
            vmem((2, groups, total, HD), BF16),
        ]
        + [dma((groups, links, subs))] * 5 + [dma((links, osubs))] * 5
        + [dma((links,))] * 2 + [dma((groups,))] * 4 + [dma((homes, 2))] * 2 + [dma((homes,))] * 2
        + [dma((2,))] * 2 + [dma((n,))] * 6,
        compiler_params=pltpu.CompilerParams(
            collective_id=0, has_side_effects=True, vmem_limit_bytes=60 * 1024 * 1024
        ),
    )(lengths, destinations, tok, q_weight, kv, o, cosine, sine)
    if not straight:
        out = out.transpose(1, 0, 2)
    projected = out.reshape(1, total, -1)
    return projected, cache.reshape(1, 2, 2 * groups, half, HD)


def solution(mesh):
    placed = (
        P(("parts", "dp"), None, None),
        P("dp", "tensor"),
        P("dp", None, "tensor"),
        P("tensor", "dp"),
        P(("parts", "dp")),
        P(("parts", "dp")),
    )
    return jax.shard_map(
        functools.partial(on_device, mesh.shape["dp"]),
        mesh=mesh,
        in_specs=placed,
        out_specs=(
            P(("parts", "dp"), None, "tensor"),
            P(("parts", "dp"), None, None, "tensor", None),
        ),
        check_vma=False,
    )
```
